32 devices in a mesh: dp: 2 (over z, core), sp: 16 (over x, y).
Axes of the slice: x: 4, y: 4, z: 1, core: 2. Of those that a mesh axis runs over, the one named last changes fastest.
The devices are a block of a 4x4x8 slice.
Arguments:
- q: bfloat16 [64, 56, 128], P('dp'), parts along dimension 0
- k: bfloat16 [64, 2048, 56, 128], P('dp', 'sp'), parts along dimension 0
- v: bfloat16 [64, 2048, 56, 128], P('dp', 'sp'), parts along dimension 0
Outputs:
- q: bfloat16 [64, 56, 128], P('dp'), parts along dimension 0
There are 2 independent parts. The reference program is written for one: setup_inputs(seed, part) draws one part's arguments, and reference() takes and returns one part's arrays. A program takes and returns all parts, laid end to end along the dimension named above; each array names one.
All inputs are finite; a program needn't handle non-finite values.
Results may differ from the reference program's by a relative error of at most 0.012.
Values are sent between devices in bfloat16 or wider.
A program may use at most 768 MiB of HBM per device.

```python
import jax
import jax.numpy as jnp

BATCH = 32
CACHE = 2048
HEADS = 56
KV_HEADS = 56
HEAD = 128


def setup_inputs(seed: int = 0, part: int = 0) -> dict:
    kq, kk, kv = (jax.random.fold_in(k, part) for k in jax.random.split(jax.random.key(seed), 3))
    return {
        "q": (3 * jax.random.normal(kq, (BATCH, HEADS, HEAD), jnp.float32)).astype(jnp.bfloat16),
        "k": jax.random.normal(kk, (BATCH, CACHE, KV_HEADS, HEAD), jnp.float32).astype(jnp.bfloat16),
        "v": jax.random.normal(kv, (BATCH, CACHE, KV_HEADS, HEAD), jnp.float32).astype(jnp.bfloat16),
    }


def einsum(form, a, b):
    return jnp.einsum(form, a.astype(jnp.float32), b.astype(jnp.float32))


def reference(q, k, v):
    grouped = q.reshape(BATCH, KV_HEADS, -1, HEAD)
    scores = einsum("bgsd,bugd->bgsu", grouped, k) * HEAD**-0.5
    weights = jax.nn.softmax(scores, -1).astype(jnp.bfloat16)
    return einsum("bgsu,bugd->bgsd", weights, v).astype(jnp.bfloat16).reshape(BATCH, HEADS, HEAD)
```

```python
import functools
import math

import jax
import jax.numpy as jnp
from jax import lax
from jax.experimental import pallas as pl
from jax.experimental.pallas import tpu as pltpu
from jax.sharding import PartitionSpec as P

MESH = pl.DeviceIdType.MESH
ROWS = 16
SLOTS = 6
LAG = 4


def attend(q2, keys, values, scale):
    twice, head = q2.shape
    lane = lax.broadcasted_iota(jnp.int32, (ROWS, 128), 1)
    row = lax.broadcasted_iota(jnp.int32, (ROWS, 128), 0)
    other = jnp.where(lane % ROWS == row, 0.0, -jnp.inf).astype(jnp.float32)
    seen, high, total = [], [], []
    for j in range(twice // ROWS):
        q = q2[j * ROWS : (j + 1) * ROWS]
        zero = jnp.zeros_like(q)
        both = jnp.concatenate([jnp.concatenate([q, zero], 1), jnp.concatenate([zero, q], 1)], 0)
        k = keys(j)
        half = k.shape[0] // 2
        k = jnp.concatenate([k[:half], k[half:]], 1)
        s = lax.dot_general(both, k, (((1,), (1,)), ((), ())), preferred_element_type=jnp.float32)
        pieces = [s[r : r + ROWS, c : c + 128] + other for r in (0, ROWS) for c in range(0, half, 128)]
        m = jnp.max(functools.reduce(jnp.maximum, pieces), -1, keepdims=True)
        w = [jnp.exp2((x - m) * scale) for x in pieces]
        total.append(jnp.sum(functools.reduce(jnp.add, w), -1, keepdims=True))
        n = half // 128
        w = jnp.concatenate([jnp.concatenate(w[:n], 1), jnp.concatenate(w[n:], 1)], 0).astype(jnp.bfloat16)
        v = values(j)
        v = jnp.concatenate([v[:half], v[half:]], 1)
        o = jnp.dot(w, v, preferred_element_type=jnp.float32)
        seen.append(o[:ROWS, :head] + o[ROWS:, head:])
        high.append(m)
    seen, high, total = (jnp.concatenate(x, 0) for x in (seen, high, total))
    heads = twice // 2
    m = jnp.maximum(high[:heads], high[heads:])
    a, b = jnp.exp2((high[:heads] - m) * scale), jnp.exp2((high[heads:] - m) * scale)
    return seen[:heads] * a + seen[heads:] * b, m, total[:heads] * a + total[heads:] * b


def kernel(side, scale, q_hbm, k_hbm, v_hbm, o_hbm, q2, kbuf, vbuf, ax, sx, ay, sy, out, ksem, vsem, qsem, osem, asend, ssend, xa, xs, ya, ys):
    n, heads, head = q_hbm.shape
    slots = kbuf.shape[0]
    me = lax.axis_index("sp")
    across, along = me // side, me % side

    def load(b):
        slot = b % slots
        return (
            pltpu.make_async_copy(k_hbm.at[b], kbuf.at[slot], ksem.at[slot]),
            pltpu.make_async_copy(v_hbm.at[b], vbuf.at[slot], vsem.at[slot]),
        )

    queries = [pltpu.make_async_copy(q_hbm, q2.at[:, pl.ds(i * heads, heads)], qsem.at[i]) for i in range(2)]
    for copy in queries:
        copy.start()
    for b in range(slots):
        for copy in load(b):
            copy.start()

    def to_x(d):
        return across * side + (along + d) % side

    def to_y(d):
        return ((across + d) % side) * side + along

    barrier = pltpu.get_barrier_semaphore()
    for d in range(1, side):
        for to in (to_x, to_y):
            pl.semaphore_signal(barrier, inc=1, device_id={"sp": to(d)}, device_id_type=MESH)
    pl.semaphore_wait(barrier, 2 * (side - 1))

    def send(b, to, phase, acc, stat, acc_sem, stat_sem):
        for d in range(1, side):
            for buf, out_sem, in_sem in ((stat, ssend, stat_sem), (acc, asend, acc_sem)):
                pltpu.make_async_remote_copy(
                    src_ref=buf.at[b, 0],
                    dst_ref=buf.at[b, d],
                    send_sem=out_sem.at[phase],
                    recv_sem=in_sem.at[b],
                    device_id={"sp": to(d)},
                    device_id_type=MESH,
                ).start()

    def arrived(b, buf, sem):
        part = buf.at[b, pl.ds(1, side - 1)]
        pltpu.make_async_copy(part, part, sem.at[b]).wait()

    eye = lax.broadcasted_iota(jnp.int32, (heads, 128), 0) == lax.broadcasted_iota(jnp.int32, (heads, 128), 1)

    def to_row(column):
        return jnp.sum(jnp.where(eye, column, 0.0), 0, keepdims=True)

    def to_column(row):
        return jnp.sum(jnp.where(eye, row, 0.0), 1, keepdims=True)

    def merged(b, acc, stat, mine, last):
        slot = [(mine - c + side) % side for c in range(side)]
        high = [stat[b, s, 0:1, :] for s in slot]
        m = functools.reduce(jnp.maximum, high)
        w = [jnp.exp2((h - m) * scale) for h in high]
        total = functools.reduce(jnp.add, [x * stat[b, s, 1:2, :] for x, s in zip(w, slot)])
        if last:
            w = [x / total for x in w]
        seen = functools.reduce(jnp.add, [to_column(x) * acc[b, s].astype(jnp.float32) for x, s in zip(w, slot)])
        return seen.astype(jnp.bfloat16), m, total

    def own(b):
        for copy in load(b):
            copy.wait()

    def work(b):
        slot = b % slots
        rows = lambda buf: lambda j: buf[slot, :, j * ROWS : (j + 1) * ROWS, :].reshape(-1, head)
        seen, m, total = attend(q2[b], rows(kbuf), rows(vbuf), scale)
        ax[b, 0] = seen.astype(jnp.bfloat16)
        sx[b, 0, 0:1, :] = to_row(m)
        sx[b, 0, 1:2, :] = to_row(total)

    def wait_x(b):
        arrived(b, ax, xa)
        arrived(b, sx, xs)

    def wait_y(b):
        arrived(b, ay, ya)
        arrived(b, sy, ys)

    def x_merge(b):
        ay[b, 0], sy[b, 0, 0:1, :], sy[b, 0, 1:2, :] = merged(b, ax, sx, along, False)

    def y_merge(b):
        out[b] = merged(b, ay, sy, across, True)[0]

    def send_x(b):
        send(b, to_x, 0, ax, sx, xa, xs)

    def send_y(b):
        send(b, to_y, 1, ay, sy, ya, ys)

    def put(b):
        pltpu.make_async_copy(out.at[b], o_hbm.at[b], osem).start()

    def step(b, x, y, more):
        own(b)
        if x:
            wait_x(b - LAG)
        if y:
            wait_y(b - 2 * LAG)
        work(b)
        if x:
            x_merge(b - LAG)
        if y:
            y_merge(b - 2 * LAG)
        send_x(b)
        if x:
            send_y(b - LAG)
        if y:
            put(b - 2 * LAG)
        if more:
            for copy in load(b + slots):
                copy.start()

    for copy in queries:
        copy.wait()

    def loop(first, end, *kinds):
        @pl.loop(first, end)
        def _(b):
            step(b, *kinds)

    loop(0, LAG, False, False, True)
    loop(LAG, 2 * LAG, True, False, True)
    loop(2 * LAG, n - slots, True, True, True)
    loop(n - slots, n, True, True, False)

    @pl.loop(n - LAG, n)
    def _(b):
        wait_x(b)
        x_merge(b)
        send_y(b)
        wait_y(b - LAG)
        y_merge(b - LAG)
        put(b - LAG)

    @pl.loop(n - LAG, n)
    def _(b):
        wait_y(b)
        y_merge(b)
        put(b)

    pltpu.make_async_copy(out, o_hbm, osem).wait()
    for phase, (acc, stat) in enumerate(((ax, sx), (ay, sy))):
        for buf, sem in ((acc, asend), (stat, ssend)):
            part = buf.at[:, pl.ds(1, side - 1)]
            pltpu.make_async_copy(part, part, sem.at[phase]).wait()


def solution(mesh):
    side = math.isqrt(mesh.shape["sp"])

    def step(q, k, v):
        n, heads, head = q.shape
        tokens = k.shape[1]
        scale = head**-0.5 * math.log2(math.e)
        k, v = (x.reshape(n, tokens // 2, 2 * heads, head) for x in (k, v))
        any_ = pl.BlockSpec(memory_space=pl.ANY)
        dma = pltpu.SemaphoreType.DMA
        return pl.pallas_call(
            functools.partial(kernel, side, scale),
            out_shape=jax.ShapeDtypeStruct(q.shape, q.dtype),
            in_specs=[any_] * 3,
            out_specs=any_,
            scratch_shapes=[
                pltpu.VMEM((n, 2 * heads, head), q.dtype),
                pltpu.VMEM((SLOTS,) + k.shape[1:], k.dtype),
                pltpu.VMEM((SLOTS,) + v.shape[1:], v.dtype),
                pltpu.VMEM((n, side, heads, head), jnp.bfloat16),
                pltpu.VMEM((n, side, 2, 128), jnp.float32),
                pltpu.VMEM((n, side, heads, head), jnp.bfloat16),
                pltpu.VMEM((n, side, 2, 128), jnp.float32),
                pltpu.VMEM((n, heads, head), q.dtype),
                dma((SLOTS,)),
                dma((SLOTS,)),
                dma((2,)),
                dma,
                dma((2,)),
                dma((2,)),
                dma((n,)),
                dma((n,)),
                dma((n,)),
                dma((n,)),
            ],
            compiler_params=pltpu.CompilerParams(
                collective_id=0, has_side_effects=True, vmem_limit_bytes=56 * 2**20
            ),
            name="decode_attention",
        )(q, k, v)

    return jax.shard_map(
        step,
        mesh=mesh,
        in_specs=(P("dp", None, None), P("dp", "sp", None, None), P("dp", "sp", None, None)),
        out_specs=P("dp", None, None),
        check_vma=False,
    )
```

```python
import functools
import math

import jax
import jax.numpy as jnp
from jax import lax
from jax.experimental import pallas as pl
from jax.experimental.pallas import tpu as pltpu
from jax.sharding import PartitionSpec as P

MESH = pl.DeviceIdType.MESH
ROWS = 8
SLOTS = 6
PAIR = 2
LAG = 6
TILES = 2
WIDE = 256


def scores(q, tile):
    k = jnp.concatenate([tile(t) for t in range(TILES)], 0)
    return lax.dot_general(q, k, (((1,), (1,)), ((), ())), preferred_element_type=jnp.float32)


def weigh(s, scale):
    lane = lax.broadcasted_iota(jnp.int32, (ROWS, 128), 1)
    row = lax.broadcasted_iota(jnp.int32, (ROWS, 128), 0)
    other = jnp.where(lane % ROWS == row, 0.0, -jnp.inf).astype(jnp.float32)
    pieces = [[s[r : r + ROWS, c : c + 128] + other for c in range(0, s.shape[1], 128)] for r in (0, ROWS)]
    m = jnp.max(functools.reduce(jnp.maximum, [y for x in pieces for y in x]), -1, keepdims=True)
    m = jnp.broadcast_to(m, (ROWS, 128))
    w = [[jnp.exp2((y - m) * scale) for y in x] for x in pieces]
    total = jnp.sum(functools.reduce(jnp.add, [y for x in w for y in x]), -1, keepdims=True)
    total = jnp.broadcast_to(total, (ROWS, 128))
    return jnp.concatenate([jnp.concatenate(x, 1) for x in w], 0).astype(jnp.bfloat16), m, total


def values_seen(weights, tile):
    v = jnp.concatenate([tile(t) for t in range(TILES)], 0)
    return jnp.dot(weights, v, preferred_element_type=jnp.float32)


def order(keys, values):
    found, k, v, done_k, done_v = [], 0, 0, 0, 0
    last = min(values, 5)
    while k < keys or v < values:
        if k < keys:
            found.append(("k", k))
            k += 1
            if k == min(2, keys):
                found.append(("m", 0))
            if k - done_k > 3:
                found.append(("K", done_k))
                done_k += 1
            due = 0 if k < 3 else (values - last) * (k - 2) // max(keys - 2, 1)
        else:
            due = v + 1
        while v < due:
            found.append(("v", v))
            v += 1
            if v - done_v > 4:
                found.append(("V", done_v))
                done_v += 1
            if k == keys and done_k < keys:
                found.append(("K", done_k))
                done_k += 1
    found += [("K", j) for j in range(done_k, keys)] + [("V", j) for j in range(done_v, values)]
    return found if keys else [("m", 0)] + found


def kernel(
    side, scale, q_hbm, k_hbm, v_hbm, o_hbm, q2, kbuf, vbuf, wbuf, part, stat, out, racc, rstat, xacc, xstat, ypart, ysent, yacc,
    ystat, eacc, estat, ewide, ksem, vsem, qsem, osem, sent_acc, sent_stat, r_acc, r_stat, g_sent, g_in, x_acc, x_stat, y_acc,
    y_stat, e_acc, e_stat,
):
    n, classes, _, head = q_hbm.shape
    heads = classes * ROWS
    slots, _, tokens, _, _ = kbuf.shape
    me = lax.axis_index("sp")
    across, along = me // side, me % side

    def load(hbm, buf, sem, b):
        pltpu.make_async_copy(hbm.at[b], buf.at[b % slots], sem.at[b % slots]).start()

    def loaded(buf, sem, b):
        part = buf.at[b % slots]
        pltpu.make_async_copy(part, part, sem.at[b % slots]).wait()

    load_k, load_v = (functools.partial(load, *x) for x in ((k_hbm, kbuf, ksem), (v_hbm, vbuf, vsem)))
    wait_k, wait_v = (functools.partial(loaded, *x) for x in ((kbuf, ksem), (vbuf, vsem)))

    queries = [
        pltpu.make_async_copy(q_hbm, q2.at[:, :, pl.ds(i * ROWS, ROWS), pl.ds(i * head, head)], qsem.at[i])
        for i in range(2)
    ]
    for copy in queries:
        copy.start()
    for b in range(slots - 1):
        load_k(b)
        if b < slots - PAIR:
            load_v(b)
    zero = jnp.zeros((classes, ROWS, head), q2.dtype)

    @pl.loop(0, n)
    def _(b):
        q2[b, :, :ROWS, head:] = zero
        q2[b, :, ROWS:, :head] = zero

    group = side * side
    square = group + group // 2
    straight = n - 2

    def device(dx, dy):
        return ((across + dx) % side) * side + (along + dy) % side

    others = sorted(((dx, dy) for dx in range(side) for dy in range(side) if dx or dy), key=lambda d: -sum(min(x, side - x) for x in d))

    barrier = pltpu.get_barrier_semaphore()
    for dx, dy in others:
        pl.semaphore_signal(barrier, inc=1, device_id={"sp": device(dx, dy)}, device_id_type=MESH)
    pl.semaphore_wait(barrier, group - 1)

    def push(src, dst, to, send_sem, recv_sem):
        pltpu.make_async_remote_copy(
            src_ref=src, dst_ref=dst, send_sem=send_sem, recv_sem=recv_sem, device_id={"sp": to}, device_id_type=MESH
        ).start()

    def wait(like, sem):
        pltpu.make_async_copy(like, like, sem).wait()

    eye = lax.broadcasted_iota(jnp.int32, (heads, 128), 0) == lax.broadcasted_iota(jnp.int32, (heads, 128), 1)

    def to_row(column):
        return jnp.sum(jnp.where(eye, column, 0.0), 0, keepdims=True)

    def to_column(row):
        column = jnp.sum(jnp.where(eye, row, 0.0), 1, keepdims=True)
        return jnp.broadcast_to(column, (heads, 128))

    def shares(high, total, last):
        m = functools.reduce(jnp.maximum, high)
        w = [jnp.exp2((h - m) * scale) for h in high]
        total = functools.reduce(jnp.add, [x * t for x, t in zip(w, total)])
        return [x / total for x in w] if last else w, m, total

    def joined(accs, stats, last):
        w, m, total = shares([x[0:1, :] for x in stats], [x[1:2, :] for x in stats], last)
        seen = functools.reduce(jnp.add, [to_column(x) * acc.astype(jnp.float32) for x, acc in zip(w, accs)])
        return seen.astype(jnp.bfloat16), m, total

    def tile_of(buf, b, j):
        def tile(t):
            size = WIDE // ROWS
            rows = [buf[b % slots, p * size : (p + 1) * size, j].reshape(WIDE, head) for p in (2 * t, 2 * t + 1)]
            return jnp.concatenate(rows, 1)

        return tile

    def work(qk, pv, merge):
        started, made, seen = {}, {}, {}
        for kind, i in order(len(qk) * classes, len(pv) * classes):
            at, j = i // classes, i % classes
            if kind == "m":
                merge()
            elif kind == "k":
                b = qk[at]
                started[kind, i] = scores(q2[b, j], tile_of(kbuf, b, j))
            elif kind == "v":
                b = pv[at]
                started[kind, i] = values_seen(wbuf[b % (2 * PAIR), j], tile_of(vbuf, b, j))
            elif kind == "K":
                b = qk[at]
                w, m, total = weigh(started["k", i], scale)
                wbuf[b % (2 * PAIR), j] = w
                made[at, j] = m, total
                if j == classes - 1:
                    m, total = (jnp.concatenate([made[at, c][x] for c in range(classes)], 0) for x in range(2))
                    stat[b, 0:1, :] = to_row(m)
                    stat[b, 1:2, :] = to_row(total)
            else:
                b = pv[at]
                o = started["v", i]
                seen[at, j] = o[:ROWS, :head] + o[ROWS:, head:]
                if j == classes - 1:
                    part[b] = jnp.concatenate([seen[at, c] for c in range(classes)], 0).astype(jnp.bfloat16)

    def owner(b):
        second = b // group
        j = b - second * group
        x, y = j // (side // 2), j % (side // 2)
        spread = x * side + 2 * y + x % 2
        return j + second * (spread - j)

    def send_owned(b):
        to = owner(b)

        @pl.when(to != me)
        def _():
            push(stat.at[b], rstat.at[b // group, me], to, sent_stat.at[0], r_stat.at[b // group])
            push(part.at[b], racc.at[b // group, me], to, sent_acc.at[0], r_acc.at[b // group])

    def put_together(g, b):
        wait(rstat.at[g, pl.ds(0, group - 1)], r_stat.at[g])
        wait(racc.at[g, pl.ds(0, group - 1)], r_acc.at[g])
        racc[g, me], rstat[g, me] = part[b], stat[b]
        out[b] = joined([racc[g, c] for c in range(group)], [rstat[g, c] for c in range(group)], True)[0]

        @pl.loop(1, group)
        def _(d):
            push(out.at[b], out.at[b], device(d // side, d % side), g_sent.at[g], g_in.at[b])

    in_second = (across + along) % 2 == 0
    mine = [me, group + across * (side // 2) + along // 2]

    def send_x(b, count):
        at = pl.ds(b - square, count)
        for d in (2, 1, 3):
            to = device(0, d)
            push(stat.at[pl.ds(b, count)], xstat.at[d, at], to, sent_stat.at[1], x_stat.at[b - square])
            push(part.at[pl.ds(b, count)], xacc.at[d, at], to, sent_acc.at[1], x_acc.at[b - square])

    def by_source(here):
        return [(here - c + side) % side for c in range(side)]

    def next_y(b, count):
        i = b - square
        at = pl.ds(i, count)
        wait(xstat.at[pl.ds(1, side - 1), at], x_stat.at[i])
        wait(xacc.at[pl.ds(1, side - 1), at], x_acc.at[i])
        for k in range(i, i + count):
            xacc[0, k], xstat[0, k] = part[k + square], stat[k + square]
            slots = by_source(along)
            ypart[k], m, total = joined([xacc[s, k] for s in slots], [xstat[s, k] for s in slots], False)
            ysent[k, 0:1, :], ysent[k, 1:2, :] = m, total
        for d in (2, 1, 3):
            to = device(d, 0)
            push(ysent.at[at], ystat.at[d, at], to, sent_stat.at[2], y_stat.at[i])
            push(ypart.at[at], yacc.at[d, at], to, sent_acc.at[2], y_acc.at[i])

    def put(b, count):
        pltpu.make_async_copy(out.at[pl.ds(b, count)], o_hbm.at[pl.ds(b, count)], osem).start()

    def end_y(b, count):
        i = b - square
        at = pl.ds(i, count)
        wait(ystat.at[pl.ds(1, side - 1), at], y_stat.at[i])
        wait(yacc.at[pl.ds(1, side - 1), at], y_acc.at[i])
        for k in range(i, i + count):
            yacc[0, k], ystat[0, k] = ypart[k], ysent[k]
            slots = by_source(across)
            out[k + square] = joined([yacc[s, k] for s in slots], [ystat[s, k] for s in slots], True)[0]
        put(b, count)

    def send_straight(b):
        for dx, dy in others:
            push(part.at[b], eacc.at[b - straight, dx * side + dy], device(dx, dy), sent_acc.at[3], e_acc.at[b - straight])

    def send_straight_stat():
        for dx, dy in others:
            push(stat.at[pl.ds(straight, 2)], estat.at[dx * side + dy], device(dx, dy), sent_stat.at[3], e_stat)

    from_all = [((across - x + side) % side) * side + (along - y + side) % side for x in range(side) for y in range(side)]

    def straight_shares():
        wait(estat.at[pl.ds(1, group - 1)], e_stat)
        for i in range(2):
            estat[0, i] = stat[straight + i]
            w, _, _ = shares([estat[s, i, 0:1, :] for s in from_all], [estat[s, i, 1:2, :] for s in from_all], True)
            for c, x in enumerate(w):
                ewide[i, c] = to_column(x)

    def end_straight(b):
        i = b - straight
        wait(eacc.at[i, pl.ds(1, group - 1)], e_acc.at[i])
        eacc[i, 0] = part[b]
        seen = [ewide[i, c] * eacc[i, s].astype(jnp.float32) for c, s in enumerate(from_all)]
        out[b] = functools.reduce(jnp.add, seen).astype(jnp.bfloat16)
        put(b, 1)

    def step(first, pv=True):
        old = first - PAIR
        for i in range(PAIR):
            wait_k(first + i)
            if pv:
                wait_v(old + i)
        work([first + i for i in range(PAIR)], [old + i for i in range(PAIR)] if pv else [], lambda: None)
        more = first + slots - PAIR
        if not pv:
            load_v(more)
            load_k(more + 1)
            load_v(more + 1)
            load_k(more + 2)
            return

        @pl.when(more < n)
        def _():
            load_v(more)
            load_k(more + 1)
            load_v(more + 1)

        @pl.when(more + 2 < n)
        def _():
            load_k(more + 2)

        @pl.when(old < square)
        def _():
            for i in range(PAIR):
                send_owned(old + i)

        @pl.when(old == group + LAG - PAIR)
        def _():
            put_together(0, mine[0])

    for copy in queries:
        copy.wait()

    step(0, pv=False)

    ahead = straight - 2

    @pl.loop(PAIR, ahead, step=PAIR)
    def _(b):
        step(b)

    send_x(ahead - 4, 2)
    wait_k(ahead)
    wait_v(ahead - 2)
    wait_v(ahead - 1)
    work([ahead], [ahead - 2, ahead - 1], lambda: None)
    send_x(ahead - 2, 2)
    for b in range(ahead + 1, n):
        wait_k(b)
        wait_v(b - 1)
        work([b], [b - 1], lambda: None)
        if b == straight:
            send_x(ahead, 2)
        if b > straight:
            send_straight(b - 1)
    wait_v(n - 1)
    work([], [n - 1], lambda: None)
    send_straight(n - 1)
    send_straight_stat()

    @pl.when(in_second)
    def _():
        put_together(1, mine[1])

    for b in range(square, straight, 2):
        next_y(b, 2)
    straight_shares()
    for b in range(square, straight, 2):
        end_y(b, 2)

    @pl.loop(0, square)
    def _(b):
        @pl.when(owner(b) != me)
        def _():
            wait(out.at[b], g_in.at[b])

    put(0, square)
    for b in range(straight, n):
        end_straight(b)

    wait(out, osem)

    @pl.when(in_second)
    def _():
        wait(part.at[pl.ds(0, square - 2)], sent_acc.at[0])
        wait(stat.at[pl.ds(0, square - 2)], sent_stat.at[0])
        wait(out.at[pl.ds(0, group - 1)], g_sent.at[1])

    @pl.when(jnp.logical_not(in_second))
    def _():
        wait(part.at[pl.ds(0, square - 1)], sent_acc.at[0])
        wait(stat.at[pl.ds(0, square - 1)], sent_stat.at[0])

    wait(out.at[pl.ds(0, group - 1)], g_sent.at[0])
    for i, (acc, st) in enumerate(((xacc, xstat), (yacc, ystat)), 1):
        wait(acc.at[pl.ds(1, side - 1)], sent_acc.at[i])
        wait(st.at[pl.ds(1, side - 1)], sent_stat.at[i])
    wait(eacc.at[:, pl.ds(1, group - 1)], sent_acc.at[3])
    wait(estat.at[pl.ds(1, group - 1)], sent_stat.at[3])


def solution(mesh):
    side = math.isqrt(mesh.shape["sp"])

    def step(q, k, v):
        n, heads, head = q.shape
        tokens = k.shape[1]
        scale = head**-0.5 * math.log2(math.e)
        q, k, v = (x.reshape(x.shape[:-2] + (heads // ROWS, ROWS, head)) for x in (q, k, v))
        held = (SLOTS, tokens, heads // ROWS, ROWS, head)
        any_ = pl.BlockSpec(memory_space=pl.ANY)
        dma = pltpu.SemaphoreType.DMA
        bf16, f32 = (lambda *shape, t=t: pltpu.VMEM(shape, t) for t in (jnp.bfloat16, jnp.float32))
        group = side * side
        turns = n - 2 - group - group // 2
        return pl.pallas_call(
            functools.partial(kernel, side, scale),
            out_shape=jax.ShapeDtypeStruct((n, heads, head), q.dtype),
            in_specs=[any_] * 3,
            out_specs=any_,
            scratch_shapes=[
                pltpu.VMEM((n, heads // ROWS, 2 * ROWS, 2 * head), q.dtype),
                pltpu.VMEM(held, k.dtype),
                pltpu.VMEM(held, v.dtype),
                pltpu.VMEM((2 * PAIR, heads // ROWS, 2 * ROWS, TILES * WIDE), jnp.bfloat16),
                bf16(n, heads, head),
                f32(n, 2, 128),
                bf16(n, heads, head),
                bf16(2, group, heads, head),
                f32(2, group, 2, 128),
                bf16(side, turns, heads, head),
                f32(side, turns, 2, 128),
                bf16(turns, heads, head),
                f32(turns, 2, 128),
                bf16(side, turns, heads, head),
                f32(side, turns, 2, 128),
                bf16(2, group, heads, head),
                f32(group, 2, 2, 128),
                f32(2, group, heads, 128),
                dma((SLOTS,)),
                dma((SLOTS,)),
                dma((2,)),
                dma,
                dma((4,)),
                dma((4,)),
                dma((2,)),
                dma((2,)),
                dma((2,)),
                dma((n - 2 - turns,)),
                dma((turns,)),
                dma((turns,)),
                dma((turns,)),
                dma((turns,)),
                dma((2,)),
                dma,
            ],
            compiler_params=pltpu.CompilerParams(
                collective_id=0, has_side_effects=True, vmem_limit_bytes=60 * 2**20
            ),
            name="decode_attention",
        )(q, k, v)

    return jax.shard_map(
        step,
        mesh=mesh,
        in_specs=(P("dp", None, None), P("dp", "sp", None, None), P("dp", "sp", None, None)),
        out_specs=P("dp", None, None),
        check_vma=False,
    )
```

```python
import functools
import math

import jax
import jax.numpy as jnp
from jax import lax
from jax.experimental import pallas as pl
from jax.experimental.pallas import tpu as pltpu
from jax.sharding import PartitionSpec as P

MESH = pl.DeviceIdType.MESH
ROWS = 8
SLOTS = 8
AHEAD = 4
STRAIGHT = 0
PAIR = 2
LAG = 6
TILES = 2
WIDE = 256


def scores(q, tile):
    k = jnp.concatenate([tile(t) for t in range(TILES)], 0)
    return lax.dot_general(q, k, (((1,), (1,)), ((), ())), preferred_element_type=jnp.float32)


def weigh(s, scale):
    lane = lax.broadcasted_iota(jnp.int32, (ROWS, 128), 1)
    row = lax.broadcasted_iota(jnp.int32, (ROWS, 128), 0)
    other = jnp.where(lane % ROWS == row, 0.0, -jnp.inf).astype(jnp.float32)
    pieces = [[s[r : r + ROWS, c : c + 128] + other for c in range(0, s.shape[1], 128)] for r in (0, ROWS)]
    m = jnp.max(functools.reduce(jnp.maximum, [y for x in pieces for y in x]), -1, keepdims=True)
    m = jnp.broadcast_to(m, (ROWS, 128))
    w = [[jnp.exp2((y - m) * scale) for y in x] for x in pieces]
    total = jnp.sum(functools.reduce(jnp.add, [y for x in w for y in x]), -1, keepdims=True)
    total = jnp.broadcast_to(total, (ROWS, 128))
    return jnp.concatenate([jnp.concatenate(x, 1) for x in w], 0).astype(jnp.bfloat16), m, total


def values_seen(weights, tile):
    v = jnp.concatenate([tile(t) for t in range(TILES)], 0)
    return jnp.dot(weights, v, preferred_element_type=jnp.float32)


def order(keys, values):
    found, k, v, done_k, done_v = [], 0, 0, 0, 0
    last = min(values, 5)
    while k < keys or v < values:
        if k < keys:
            found.append(("k", k))
            k += 1
            if k == min(2, keys):
                found.append(("m", 0))
            if k - done_k > 3:
                found.append(("K", done_k))
                done_k += 1
            due = 0 if k < 3 else (values - last) * (k - 2) // max(keys - 2, 1)
        else:
            due = v + 1
        while v < due:
            found.append(("v", v))
            v += 1
            if v - done_v > 4:
                found.append(("V", done_v))
                done_v += 1
            if k == keys and done_k < keys:
                found.append(("K", done_k))
                done_k += 1
    found += [("K", j) for j in range(done_k, keys)] + [("V", j) for j in range(done_v, values)]
    return found if keys else [("m", 0)] + found


def kernel(
    side, scale, q_hbm, k_hbm, v_hbm, out, q2, kbuf, vbuf, wbuf, part, stat, racc, rstat, xacc, xstat, ypart, ysent, yacc,
    ystat, eacc, estat, ewide, ksem, vsem, qsem, sent_acc, sent_stat, r_acc, r_stat, g_sent, g_in, x_acc, x_stat, y_acc,
    y_stat, e_acc, e_stat,
):
    n, classes, _, head = q_hbm.shape
    heads = classes * ROWS
    slots, _, tokens, _, _ = kbuf.shape
    me = lax.axis_index("sp")
    across, along = me // side, me % side

    group = side * side
    square = group + group // 2

    def sequence(turn):
        turned = jnp.where(turn < group, (turn + me) % group, group + (turn + me) % (group // 2))
        return jnp.where(turn < square, turned, turn)

    def load(hbm, buf, sem, b):
        pltpu.make_async_copy(hbm.at[sequence(b)], buf.at[b % slots], sem.at[b % slots]).start()

    def loaded(buf, sem, b):
        part = buf.at[b % slots]
        pltpu.make_async_copy(part, part, sem.at[b % slots]).wait()

    load_k, load_v = (functools.partial(load, *x) for x in ((k_hbm, kbuf, ksem), (v_hbm, vbuf, vsem)))
    wait_k, wait_v = (functools.partial(loaded, *x) for x in ((kbuf, ksem), (vbuf, vsem)))

    queries = [
        pltpu.make_async_copy(q_hbm, q2.at[:, :, pl.ds(i * ROWS, ROWS), pl.ds(i * head, head)], qsem.at[i])
        for i in range(2)
    ]
    for copy in queries:
        copy.start()
    for b in range(slots):
        if b >= AHEAD:
            load_v(b - AHEAD)
        load_k(b)
    zero = jnp.zeros((classes, ROWS, head), q2.dtype)

    @pl.loop(0, n)
    def _(b):
        q2[b, :, :ROWS, head:] = zero
        q2[b, :, ROWS:, :head] = zero

    straight = n - STRAIGHT

    def device(dx, dy):
        return ((across + dx) % side) * side + (along + dy) % side

    others = sorted(((dx, dy) for dx in range(side) for dy in range(side) if dx or dy), key=lambda d: -sum(min(x, side - x) for x in d))

    barrier = pltpu.get_barrier_semaphore()
    for dx, dy in others:
        pl.semaphore_signal(barrier, inc=1, device_id={"sp": device(dx, dy)}, device_id_type=MESH)

    def push(src, dst, to, send_sem, recv_sem):
        pltpu.make_async_remote_copy(
            src_ref=src, dst_ref=dst, send_sem=send_sem, recv_sem=recv_sem, device_id={"sp": to}, device_id_type=MESH
        ).start()

    def wait(like, sem):
        pltpu.make_async_copy(like, like, sem).wait()

    eye = lax.broadcasted_iota(jnp.int32, (heads, 128), 0) == lax.broadcasted_iota(jnp.int32, (heads, 128), 1)

    def to_row(column):
        return jnp.sum(jnp.where(eye, column, 0.0), 0, keepdims=True)

    def to_column(row):
        column = jnp.sum(jnp.where(eye, row, 0.0), 1, keepdims=True)
        return jnp.broadcast_to(column, (heads, 128))

    def shares(high, total, last):
        m = functools.reduce(jnp.maximum, high)
        w = [jnp.exp2((h - m) * scale) for h in high]
        total = functools.reduce(jnp.add, [x * t for x, t in zip(w, total)])
        return [x / total for x in w] if last else w, m, total

    def joined(accs, stats, last):
        w, m, total = shares([x[0:1, :] for x in stats], [x[1:2, :] for x in stats], last)
        seen = functools.reduce(jnp.add, [to_column(x) * acc.astype(jnp.float32) for x, acc in zip(w, accs)])
        return seen.astype(jnp.bfloat16), m, total

    def tile_of(buf, b, j):
        def tile(t):
            size = WIDE // ROWS
            rows = [buf[b % slots, p * size : (p + 1) * size, j].reshape(WIDE, head) for p in (2 * t, 2 * t + 1)]
            return jnp.concatenate(rows, 1)

        return tile

    def work(qk, pv, merge):
        started, made, seen = {}, {}, {}
        for kind, i in order(len(qk) * classes, len(pv) * classes):
            at, j = i // classes, i % classes
            if kind == "m":
                merge()
            elif kind == "k":
                b = qk[at]
                started[kind, i] = scores(q2[sequence(b), j], tile_of(kbuf, b, j))
            elif kind == "v":
                b = pv[at]
                started[kind, i] = values_seen(wbuf[b % (2 * AHEAD), j], tile_of(vbuf, b, j))
            elif kind == "K":
                b = qk[at]
                w, m, total = weigh(started["k", i], scale)
                wbuf[b % (2 * AHEAD), j] = w
                made[at, j] = m, total
                if j == classes - 1:
                    m, total = (jnp.concatenate([made[at, c][x] for c in range(classes)], 0) for x in range(2))
                    stat[b, 0:1, :] = to_row(m)
                    stat[b, 1:2, :] = to_row(total)
            else:
                b = pv[at]
                o = started["v", i]
                seen[at, j] = o[:ROWS, :head] + o[ROWS:, head:]
                if j == classes - 1:
                    part[b] = jnp.concatenate([seen[at, c] for c in range(classes)], 0).astype(jnp.bfloat16)

    def owner(b):
        second = b // group
        j = b - second * group
        x, y = j // (side // 2), j % (side // 2)
        spread = x * side + 2 * y + x % 2
        return j + second * (spread - j)

    def send_owned(b):
        to = owner(sequence(b))

        @pl.when(to != me)
        def _():
            push(stat.at[b], rstat.at[b // group, me], to, sent_stat.at[0], r_stat.at[b // group])
            push(part.at[b], racc.at[b // group, me], to, sent_acc.at[0], r_acc.at[b // group])

    def put_together(g, b):
        turn = g * group + (b - me) % (group // (g + 1))
        wait(rstat.at[g, pl.ds(0, group - 1)], r_stat.at[g])
        wait(racc.at[g, pl.ds(0, group - 1)], r_acc.at[g])
        racc[g, me], rstat[g, me] = part[turn], stat[turn]
        out[b] = joined([racc[g, c] for c in range(group)], [rstat[g, c] for c in range(group)], True)[0]

        @pl.loop(1, group)
        def _(d):
            push(out.at[b], out.at[b], device(d // side, d % side), g_sent.at[g], g_in.at[b])

    in_second = (across + along) % 2 == 0
    mine = [me, group + across * (side // 2) + along // 2]

    def send_x(b, count):
        at = pl.ds(b - square, count)
        for d in (2, 1, 3):
            to = device(0, d)
            push(stat.at[pl.ds(b, count)], xstat.at[d, at], to, sent_stat.at[1], x_stat.at[b - square])
            push(part.at[pl.ds(b, count)], xacc.at[d, at], to, sent_acc.at[1], x_acc.at[b - square])

    def by_source(here):
        return [(here - c + side) % side for c in range(side)]

    def next_y(b, count):
        i = b - square
        at = pl.ds(i, count)
        wait(xstat.at[pl.ds(1, side - 1), at], x_stat.at[i])
        wait(xacc.at[pl.ds(1, side - 1), at], x_acc.at[i])
        for k in range(i, i + count):
            xacc[0, k], xstat[0, k] = part[k + square], stat[k + square]
            slots = by_source(along)
            ypart[k], m, total = joined([xacc[s, k] for s in slots], [xstat[s, k] for s in slots], False)
            ysent[k, 0:1, :], ysent[k, 1:2, :] = m, total
        for d in (2, 1, 3):
            to = device(d, 0)
            push(ysent.at[at], ystat.at[d, at], to, sent_stat.at[2], y_stat.at[i])
            push(ypart.at[at], yacc.at[d, at], to, sent_acc.at[2], y_acc.at[i])

    def end_y(b, count):
        i = b - square
        at = pl.ds(i, count)
        wait(ystat.at[pl.ds(1, side - 1), at], y_stat.at[i])
        wait(yacc.at[pl.ds(1, side - 1), at], y_acc.at[i])
        for k in range(i, i + count):
            yacc[0, k], ystat[0, k] = ypart[k], ysent[k]
            slots = by_source(across)
            out[k + square] = joined([yacc[s, k] for s in slots], [ystat[s, k] for s in slots], True)[0]

    def send_straight(b):
        for dx, dy in others:
            push(part.at[b], eacc.at[b - straight, dx * side + dy], device(dx, dy), sent_acc.at[3], e_acc.at[b - straight])

    def send_straight_stat():
        for dx, dy in others:
            push(stat.at[pl.ds(straight, STRAIGHT)], estat.at[dx * side + dy], device(dx, dy), sent_stat.at[3], e_stat)

    from_all = [((across - x + side) % side) * side + (along - y + side) % side for x in range(side) for y in range(side)]

    def straight_shares():
        wait(estat.at[pl.ds(1, group - 1)], e_stat)
        for i in range(STRAIGHT):
            estat[0, i] = stat[straight + i]
            w, _, _ = shares([estat[s, i, 0:1, :] for s in from_all], [estat[s, i, 1:2, :] for s in from_all], True)
            for c, x in enumerate(w):
                ewide[i, c] = to_column(x)

    def end_straight(b):
        i = b - straight
        wait(eacc.at[i, pl.ds(1, group - 1)], e_acc.at[i])
        eacc[i, 0] = part[b]
        seen = [ewide[i, c] * eacc[i, s].astype(jnp.float32) for c, s in enumerate(from_all)]
        out[b] = functools.reduce(jnp.add, seen).astype(jnp.bfloat16)

    def step(first, pv=True):
        old = first - AHEAD
        for i in range(PAIR):
            wait_k(first + i)
            if pv:
                wait_v(old + i)
        work([first + i for i in range(PAIR)], [old + i for i in range(PAIR)] if pv else [], lambda: None)

        def more(i):
            load_v(old + slots + i)

            @pl.when(first + slots + i < n)
            def _():
                load_k(first + slots + i)

        if not pv:
            for i in range(PAIR):
                more(i)
            return

        @pl.when(old + slots < n)
        def _():
            for i in range(PAIR):
                more(i)

        @pl.when(old < square)
        def _():
            for i in range(PAIR):
                send_owned(old + i)

        @pl.when(old == group + LAG - PAIR)
        def _():
            put_together(0, mine[0])

    for copy in queries:
        copy.wait()

    @pl.loop(0, AHEAD, step=PAIR)
    def _(b):
        step(b, pv=False)

    pl.semaphore_wait(barrier, group - 1)

    @pl.loop(AHEAD, n - PAIR, step=PAIR)
    def _(b):
        step(b)

    turns = [(square, 2)]
    send_x(*turns[-1])
    for qk, pv in (([n - 2], [n - 6, n - 5]), ([n - 1], [n - 4]), ([], [n - 3, n - 2]), ([], [n - 1])):
        for b in qk:
            wait_k(b)
        for b in pv:
            wait_v(b)
        work(qk, pv, lambda: None)
        if pv[-1] < straight:
            turns.append((pv[0], len(pv)))
            send_x(*turns[-1])
        else:
            send_straight(n - 1)
            send_straight_stat()

    @pl.when(in_second)
    def _():
        put_together(1, mine[1])

    for turn in turns:
        next_y(*turn)
    if STRAIGHT:
        straight_shares()
    for turn in turns[:-1]:
        end_y(*turn)

    @pl.loop(0, square)
    def _(b):
        @pl.when(owner(b) != me)
        def _():
            wait(out.at[b], g_in.at[b])

    end_y(*turns[-1])
    for b in range(straight, n):
        end_straight(b)

    @pl.when(in_second)
    def _():
        wait(part.at[pl.ds(0, square - 2)], sent_acc.at[0])
        wait(stat.at[pl.ds(0, square - 2)], sent_stat.at[0])
        wait(out.at[pl.ds(0, group - 1)], g_sent.at[1])

    @pl.when(jnp.logical_not(in_second))
    def _():
        wait(part.at[pl.ds(0, square - 1)], sent_acc.at[0])
        wait(stat.at[pl.ds(0, square - 1)], sent_stat.at[0])

    wait(out.at[pl.ds(0, group - 1)], g_sent.at[0])
    for i, (acc, st) in enumerate(((xacc, xstat), (yacc, ystat)), 1):
        wait(acc.at[pl.ds(1, side - 1)], sent_acc.at[i])
        wait(st.at[pl.ds(1, side - 1)], sent_stat.at[i])
    if STRAIGHT:
        wait(eacc.at[:, pl.ds(1, group - 1)], sent_acc.at[3])
        wait(estat.at[pl.ds(1, group - 1)], sent_stat.at[3])


def solution(mesh):
    side = math.isqrt(mesh.shape["sp"])

    def step(q, k, v):
        n, heads, head = q.shape
        tokens = k.shape[1]
        scale = head**-0.5 * math.log2(math.e)
        q, k, v = (x.reshape(x.shape[:-2] + (heads // ROWS, ROWS, head)) for x in (q, k, v))
        held = (SLOTS, tokens, heads // ROWS, ROWS, head)
        any_ = pl.BlockSpec(memory_space=pl.ANY)
        dma = pltpu.SemaphoreType.DMA
        bf16, f32 = (lambda *shape, t=t: pltpu.VMEM(shape, t) for t in (jnp.bfloat16, jnp.float32))
        group = side * side
        turns = n - STRAIGHT - group - group // 2
        held_out = pl.pallas_call(
            functools.partial(kernel, side, scale),
            out_shape=jax.ShapeDtypeStruct((n + 1, heads, head), q.dtype),
            in_specs=[pl.BlockSpec(memory_space=pltpu.HBM)] * 3,
            out_specs=pl.BlockSpec(memory_space=pltpu.VMEM),
            scratch_shapes=[
                pltpu.VMEM((n, heads // ROWS, 2 * ROWS, 2 * head), q.dtype),
                pltpu.VMEM(held, k.dtype),
                pltpu.VMEM(held, v.dtype),
                pltpu.VMEM((2 * AHEAD, heads // ROWS, 2 * ROWS, TILES * WIDE), jnp.bfloat16),
                bf16(n, heads, head),
                f32(n, 2, 128),
                bf16(2, group, heads, head),
                f32(2, group, 2, 128),
                bf16(side, turns, heads, head),
                f32(side, turns, 2, 128),
                bf16(turns, heads, head),
                f32(turns, 2, 128),
                bf16(side, turns, heads, head),
                f32(side, turns, 2, 128),
                bf16(max(STRAIGHT, 1), group, heads, head),
                f32(group, max(STRAIGHT, 1), 2, 128),
                f32(max(STRAIGHT, 1), group, heads, 128),
                dma((SLOTS,)),
                dma((SLOTS,)),
                dma((2,)),
                dma((4,)),
                dma((4,)),
                dma((2,)),
                dma((2,)),
                dma((2,)),
                dma((group + group // 2,)),
                dma((turns,)),
                dma((turns,)),
                dma((turns,)),
                dma((turns,)),
                dma((2,)),
                dma,
            ],
            compiler_params=pltpu.CompilerParams(
                collective_id=0, has_side_effects=True, vmem_limit_bytes=46 * 2**20
            ),
            name="decode_attention",
        )(*(pltpu.with_memory_space_constraint(x, pltpu.HBM) for x in (q, k, v)))
        return held_out[:n]

    return jax.shard_map(
        step,
        mesh=mesh,
        in_specs=(P("dp", None, None), P("dp", "sp", None, None), P("dp", "sp", None, None)),
        out_specs=P("dp", None, None),
        check_vma=False,
    )
```

```python
import functools
import math

import jax
import jax.numpy as jnp
from jax import lax
from jax.experimental import pallas as pl
from jax.experimental.pallas import tpu as pltpu
from jax.sharding import PartitionSpec as P

MESH = pl.DeviceIdType.MESH
ROWS = 8
SLOTS = 8
AHEAD = 4
STRAIGHT = 0
PAIR = 2
LAG = 6
TILES = 2
WIDE = 256


def scores(q, tile):
    k = jnp.concatenate([tile(t) for t in range(TILES)], 0)
    return lax.dot_general(q, k, (((1,), (1,)), ((), ())), preferred_element_type=jnp.float32)


def weigh(s, scale):
    lane = lax.broadcasted_iota(jnp.int32, (ROWS, 128), 1)
    row = lax.broadcasted_iota(jnp.int32, (ROWS, 128), 0)
    other = jnp.where(lane % ROWS == row, 0.0, -jnp.inf).astype(jnp.float32)
    pieces = [[s[r : r + ROWS, c : c + 128] + other for c in range(0, s.shape[1], 128)] for r in (0, ROWS)]
    m = jnp.max(functools.reduce(jnp.maximum, [y for x in pieces for y in x]), -1, keepdims=True)
    m = jnp.broadcast_to(m, (ROWS, 128))
    w = [[jnp.exp2((y - m) * scale) for y in x] for x in pieces]
    total = jnp.sum(functools.reduce(jnp.add, [y for x in w for y in x]), -1, keepdims=True)
    total = jnp.broadcast_to(total, (ROWS, 128))
    return jnp.concatenate([jnp.concatenate(x, 1) for x in w], 0).astype(jnp.bfloat16), m, total


def values_seen(weights, tile):
    v = jnp.concatenate([tile(t) for t in range(TILES)], 0)
    return jnp.dot(weights, v, preferred_element_type=jnp.float32)


def order(keys, values):
    found, k, v, done_k, done_v = [], 0, 0, 0, 0
    last = min(values, 5)
    while k < keys or v < values:
        if k < keys:
            found.append(("k", k))
            k += 1
            if k == min(2, keys):
                found.append(("m", 0))
            if k - done_k > 3:
                found.append(("K", done_k))
                done_k += 1
            due = 0 if k < 3 else (values - last) * (k - 2) // max(keys - 2, 1)
        else:
            due = v + 1
        while v < due:
            found.append(("v", v))
            v += 1
            if v - done_v > 4:
                found.append(("V", done_v))
                done_v += 1
            if k == keys and done_k < keys:
                found.append(("K", done_k))
                done_k += 1
    found += [("K", j) for j in range(done_k, keys)] + [("V", j) for j in range(done_v, values)]
    return found if keys else [("m", 0)] + found


def kernel(
    side, scale, q_hbm, k_hbm, v_hbm, out, q2, kbuf, vbuf, wbuf, part, stat, racc, rstat, xacc, xstat, ypart, ysent, yacc,
    ystat, eacc, estat, ewide, ksem, vsem, qsem, sent_acc, sent_stat, r_acc, r_stat, g_sent, g_in, x_acc, x_stat, y_acc,
    y_stat, e_acc, e_stat,
):
    n, classes, _, head = q_hbm.shape
    heads = classes * ROWS
    slots, _, tokens, _, _ = kbuf.shape
    me = lax.axis_index("sp")
    across, along = me // side, me % side

    group = side * side
    square = group + group // 2

    def sequence(turn):
        turned = jnp.where(turn < group, (turn + me) % group, group + (turn + me) % (group // 2))
        return jnp.where(turn < square, turned, turn)

    def load(hbm, buf, sem, b):
        pltpu.make_async_copy(hbm.at[sequence(b)], buf.at[b % slots], sem.at[b % slots]).start()

    def loaded(buf, sem, b):
        part = buf.at[b % slots]
        pltpu.make_async_copy(part, part, sem.at[b % slots]).wait()

    load_k, load_v = (functools.partial(load, *x) for x in ((k_hbm, kbuf, ksem), (v_hbm, vbuf, vsem)))
    wait_k, wait_v = (functools.partial(loaded, *x) for x in ((kbuf, ksem), (vbuf, vsem)))

    queries = [
        pltpu.make_async_copy(q_hbm, q2.at[:, :, pl.ds(i * ROWS, ROWS), pl.ds(i * head, head)], qsem.at[i])
        for i in range(2)
    ]
    for copy in queries:
        copy.start()
    for b in range(slots):
        if b >= AHEAD:
            load_v(b - AHEAD)
        load_k(b)
    zero = jnp.zeros((classes, ROWS, head), q2.dtype)

    @pl.loop(0, n)
    def _(b):
        q2[b, :, :ROWS, head:] = zero
        q2[b, :, ROWS:, :head] = zero

    straight = n - STRAIGHT

    def device(dx, dy):
        return ((across + dx) % side) * side + (along + dy) % side

    others = sorted(((dx, dy) for dx in range(side) for dy in range(side) if dx or dy), key=lambda d: -sum(min(x, side - x) for x in d))

    barrier = pltpu.get_barrier_semaphore()
    for dx, dy in others:
        pl.semaphore_signal(barrier, inc=1, device_id={"sp": device(dx, dy)}, device_id_type=MESH)

    def push(src, dst, to, send_sem, recv_sem):
        pltpu.make_async_remote_copy(
            src_ref=src, dst_ref=dst, send_sem=send_sem, recv_sem=recv_sem, device_id={"sp": to}, device_id_type=MESH
        ).start()

    def wait(like, sem):
        pltpu.make_async_copy(like, like, sem).wait()

    eye = lax.broadcasted_iota(jnp.int32, (heads, 128), 0) == lax.broadcasted_iota(jnp.int32, (heads, 128), 1)

    def to_row(column):
        return jnp.sum(jnp.where(eye, column, 0.0), 0, keepdims=True)

    def to_column(row):
        column = jnp.sum(jnp.where(eye, row, 0.0), 1, keepdims=True)
        return jnp.broadcast_to(column, (heads, 128))

    def shares(high, total, last):
        m = functools.reduce(jnp.maximum, high)
        w = [jnp.exp2((h - m) * scale) for h in high]
        total = functools.reduce(jnp.add, [x * t for x, t in zip(w, total)])
        return [x / total for x in w] if last else w, m, total

    def joined(accs, stats, last):
        w, m, total = shares([x[0:1, :] for x in stats], [x[1:2, :] for x in stats], last)
        seen = functools.reduce(jnp.add, [to_column(x) * acc.astype(jnp.float32) for x, acc in zip(w, accs)])
        return seen.astype(jnp.bfloat16), m, total

    def tile_of(buf, b, j):
        def tile(t):
            size = WIDE // ROWS
            rows = [buf[b % slots, p * size : (p + 1) * size, j].reshape(WIDE, head) for p in (2 * t, 2 * t + 1)]
            return jnp.concatenate(rows, 1)

        return tile

    def work(qk, pv, merge):
        started, made, seen = {}, {}, {}
        for kind, i in order(len(qk) * classes, len(pv) * classes):
            at, j = i // classes, i % classes
            if kind == "m":
                merge()
            elif kind == "k":
                b = qk[at]
                started[kind, i] = scores(q2[sequence(b), j], tile_of(kbuf, b, j))
            elif kind == "v":
                b = pv[at]
                started[kind, i] = values_seen(wbuf[b % (2 * AHEAD), j], tile_of(vbuf, b, j))
            elif kind == "K":
                b = qk[at]
                w, m, total = weigh(started["k", i], scale)
                wbuf[b % (2 * AHEAD), j] = w
                made[at, j] = m, total
                if j == classes - 1:
                    m, total = (jnp.concatenate([made[at, c][x] for c in range(classes)], 0) for x in range(2))
                    stat[b, 0:1, :] = to_row(m)
                    stat[b, 1:2, :] = to_row(total)
            else:
                b = pv[at]
                o = started["v", i]
                seen[at, j] = o[:ROWS, :head] + o[ROWS:, head:]
                if j == classes - 1:
                    part[b] = jnp.concatenate([seen[at, c] for c in range(classes)], 0).astype(jnp.bfloat16)

    def owner(b):
        second = b // group
        j = b - second * group
        x, y = j // (side // 2), j % (side // 2)
        spread = x * side + 2 * y + x % 2
        return j + second * (spread - j)

    def send_owned(b):
        to = owner(sequence(b))

        @pl.when(to != me)
        def _():
            push(stat.at[b], rstat.at[b // group, me], to, sent_stat.at[0], r_stat.at[b // group])
            push(part.at[b], racc.at[b // group, me], to, sent_acc.at[0], r_acc.at[b // group])

    def put_together(g, b):
        turn = g * group + (b - me) % (group // (g + 1))
        wait(rstat.at[g, pl.ds(0, group - 1)], r_stat.at[g])
        wait(racc.at[g, pl.ds(0, group - 1)], r_acc.at[g])
        racc[g, me], rstat[g, me] = part[turn], stat[turn]
        out[b] = joined([racc[g, c] for c in range(group)], [rstat[g, c] for c in range(group)], True)[0]

        @pl.loop(1, group)
        def _(d):
            push(out.at[b], out.at[b], device(d // side, d % side), g_sent.at[g], g_in.at[b])

    in_second = (across + along) % 2 == 0
    mine = [me, group + across * (side // 2) + along // 2]

    def send_x(b, count):
        for d in (2, 1, 3):
            to, at = device(0, d), pl.ds(b - square, count)
            push(part.at[pl.ds(b, count)], xacc.at[d, at], to, sent_acc.at[1], x_acc.at[b - square])

    def send_x_stat(b, count):
        for d in (2, 1, 3):
            to, at = device(0, d), pl.ds(b - square, count)
            push(stat.at[pl.ds(b, count)], xstat.at[d, at], to, sent_stat.at[1], x_stat.at[b - square])

    def by_source(here):
        return [(here - c + side) % side for c in range(side)]

    def summed(accs, columns):
        seen = functools.reduce(jnp.add, [w * acc.astype(jnp.float32) for w, acc in zip(columns, accs)])
        return seen.astype(jnp.bfloat16)

    def next_y(b, count):
        i = b - square
        at = pl.ds(i, count)
        slots = by_source(along)
        columns = []
        wait(xstat.at[pl.ds(1, side - 1), at], x_stat.at[i])
        for k in range(i, i + count):
            xstat[0, k] = stat[k + square]
            w, m, total = shares([xstat[s, k, 0:1, :] for s in slots], [xstat[s, k, 1:2, :] for s in slots], False)
            ysent[k, 0:1, :], ysent[k, 1:2, :] = m, total
            columns.append([to_column(x) for x in w])
        for d in (2, 1, 3):
            push(ysent.at[at], ystat.at[d, at], device(d, 0), sent_stat.at[2], y_stat.at[i])

        def finish():
            wait(xacc.at[pl.ds(1, side - 1), at], x_acc.at[i])
            for k in range(i, i + count):
                xacc[0, k] = part[k + square]
                ypart[k] = summed([xacc[s, k] for s in slots], columns[k - i])
            for d in (2, 1, 3):
                push(ypart.at[at], yacc.at[d, at], device(d, 0), sent_acc.at[2], y_acc.at[i])

        return finish

    def end_y(b, count):
        i = b - square
        at = pl.ds(i, count)
        slots = by_source(across)
        columns = []
        wait(ystat.at[pl.ds(1, side - 1), at], y_stat.at[i])
        for k in range(i, i + count):
            ystat[0, k] = ysent[k]
            w, _, _ = shares([ystat[s, k, 0:1, :] for s in slots], [ystat[s, k, 1:2, :] for s in slots], True)
            columns.append([to_column(x) for x in w])

        def finish():
            wait(yacc.at[pl.ds(1, side - 1), at], y_acc.at[i])
            for k in range(i, i + count):
                yacc[0, k] = ypart[k]
                out[k + square] = summed([yacc[s, k] for s in slots], columns[k - i])

        return finish

    def step(first, pv=True):
        old = first - AHEAD
        for i in range(PAIR):
            wait_k(first + i)
            if pv:
                wait_v(old + i)
        work([first + i for i in range(PAIR)], [old + i for i in range(PAIR)] if pv else [], lambda: None)

        def more(i):
            load_v(old + slots + i)

            @pl.when(first + slots + i < n)
            def _():
                load_k(first + slots + i)

        if not pv:
            for i in range(PAIR):
                more(i)
            return

        @pl.when(old + slots < n)
        def _():
            for i in range(PAIR):
                more(i)

        @pl.when(old < square)
        def _():
            for i in range(PAIR):
                send_owned(old + i)

        @pl.when(old == group + LAG - PAIR)
        def _():
            put_together(0, mine[0])

    for copy in queries:
        copy.wait()

    @pl.loop(0, AHEAD, step=PAIR)
    def _(b):
        step(b, pv=False)

    pl.semaphore_wait(barrier, group - 1)

    @pl.loop(AHEAD, n - PAIR, step=PAIR)
    def _(b):
        step(b)

    turns = [(square, 2), (square + 2, 2), (square + 4, 1), (square + 5, 2), (square + 7, 1)]
    for turn in turns[:3]:
        send_x_stat(*turn)
    send_x(*turns[0])
    for qk, turn in zip(([n - 2], [n - 1], [], []), turns[1:]):
        pv = [turn[0] + i for i in range(turn[1])]
        for b in qk:
            wait_k(b)
        for b in pv:
            wait_v(b)
        work(qk, pv, lambda: None)
        send_x(*turn)
        if qk:
            send_x_stat(*turns[3 + qk[0] - (n - 2)])

    @pl.when(in_second)
    def _():
        put_together(1, mine[1])

    def in_turn(act):
        for turn in turns[:3]:
            act(*turn)()
        return [act(*turn) for turn in turns[3:]]

    for finish in in_turn(next_y):
        finish()
    last = in_turn(end_y)

    @pl.loop(0, square)
    def _(b):
        @pl.when(owner(b) != me)
        def _():
            wait(out.at[b], g_in.at[b])

    for finish in last:
        finish()

    @pl.when(in_second)
    def _():
        wait(part.at[pl.ds(0, square - 2)], sent_acc.at[0])
        wait(stat.at[pl.ds(0, square - 2)], sent_stat.at[0])
        wait(out.at[pl.ds(0, group - 1)], g_sent.at[1])

    @pl.when(jnp.logical_not(in_second))
    def _():
        wait(part.at[pl.ds(0, square - 1)], sent_acc.at[0])
        wait(stat.at[pl.ds(0, square - 1)], sent_stat.at[0])

    wait(out.at[pl.ds(0, group - 1)], g_sent.at[0])
    for i, (acc, st) in enumerate(((xacc, xstat), (yacc, ystat)), 1):
        wait(acc.at[pl.ds(1, side - 1)], sent_acc.at[i])
        wait(st.at[pl.ds(1, side - 1)], sent_stat.at[i])


def solution(mesh):
    side = math.isqrt(mesh.shape["sp"])

    def step(q, k, v):
        n, heads, head = q.shape
        tokens = k.shape[1]
        scale = head**-0.5 * math.log2(math.e)
        q, k, v = (x.reshape(x.shape[:-2] + (heads // ROWS, ROWS, head)) for x in (q, k, v))
        held = (SLOTS, tokens, heads // ROWS, ROWS, head)
        any_ = pl.BlockSpec(memory_space=pl.ANY)
        dma = pltpu.SemaphoreType.DMA
        bf16, f32 = (lambda *shape, t=t: pltpu.VMEM(shape, t) for t in (jnp.bfloat16, jnp.float32))
        group = side * side
        turns = n - STRAIGHT - group - group // 2
        held_out = pl.pallas_call(
            functools.partial(kernel, side, scale),
            out_shape=jax.ShapeDtypeStruct((n + 1, heads, head), q.dtype),
            in_specs=[pl.BlockSpec(memory_space=pltpu.HBM)] * 3,
            out_specs=pl.BlockSpec(memory_space=pltpu.VMEM),
            scratch_shapes=[
                pltpu.VMEM((n, heads // ROWS, 2 * ROWS, 2 * head), q.dtype),
                pltpu.VMEM(held, k.dtype),
                pltpu.VMEM(held, v.dtype),
                pltpu.VMEM((2 * AHEAD, heads // ROWS, 2 * ROWS, TILES * WIDE), jnp.bfloat16),
                bf16(n, heads, head),
                f32(n, 2, 128),
                bf16(2, group, heads, head),
                f32(2, group, 2, 128),
                bf16(side, turns, heads, head),
                f32(side, turns, 2, 128),
                bf16(turns, heads, head),
                f32(turns, 2, 128),
                bf16(side, turns, heads, head),
                f32(side, turns, 2, 128),
                bf16(max(STRAIGHT, 1), group, heads, head),
                f32(group, max(STRAIGHT, 1), 2, 128),
                f32(max(STRAIGHT, 1), group, heads, 128),
                dma((SLOTS,)),
                dma((SLOTS,)),
                dma((2,)),
                dma((4,)),
                dma((4,)),
                dma((2,)),
                dma((2,)),
                dma((2,)),
                dma((group + group // 2,)),
                dma((turns,)),
                dma((turns,)),
                dma((turns,)),
                dma((turns,)),
                dma((2,)),
                dma,
            ],
            compiler_params=pltpu.CompilerParams(
                collective_id=0, has_side_effects=True, vmem_limit_bytes=46 * 2**20
            ),
            name="decode_attention",
        )(*(pltpu.with_memory_space_constraint(x, pltpu.HBM) for x in (q, k, v)))
        return held_out[:n]

    return jax.shard_map(
        step,
        mesh=mesh,
        in_specs=(P("dp", None, None), P("dp", "sp", None, None), P("dp", "sp", None, None)),
        out_specs=P("dp", None, None),
        check_vma=False,
    )
```
